128 devices in a mesh: row: 8 (over x_hi, y), col: 16 (over z, x_lo, core).
Axes of the slice: x: 4 (x_hi: 2, x_lo: 2; x = x_hi * 2 + x_lo), y: 4, z: 4, core: 2. Of those that a mesh axis runs over, the one named last changes fastest.
Arguments:
- left_matrix: bfloat16 [6144, 32768], P('row', 'col'), may hold values from -6 to 6
- right_matrix: bfloat16 [32768, 8192], P('row', 'col'), may hold values from -0.078125 to 0.078125
- left_mask: int32 [48, 256], P('row', 'col'), may hold values from 0 to 1
- right_mask: int32 [256, 64], P('row', 'col'), may hold values from 0 to 1
- keep_mask: int32 [48, 64], P('row', 'col'), may hold values 0 or 1
Outputs:
- product: bfloat16 [6144, 8192], P('row', 'col')
The draws below stay inside these ranges and needn't reach their ends.
All inputs are finite; a program needn't handle non-finite values. No bound on the sum of `keep_mask` on one device may be relied on, other than what follows from the above.
Results may differ from the reference program's by a relative error of at most 0.001.
Values may be sent and summed in bfloat16 or wider, within the bound.
No kernel may reach another device: no remote copies, remote signals or barrier semaphores. Data moves between devices by JAX's collectives and lax.ppermute only.
A program may use at most 128 MiB of HBM per device.

```python
import jax
import jax.numpy as jnp

ORDER = 32768
BLOCK = 128
TICKS = 3
MR_DEV = 768
NC_DEV = 512
M = 6144
N = 8192
MB = 48
KB = 256
NB = 64
UNIT = 4096
N_ROW = 8


def banded(key, rows, cols):
    row_pos = jnp.arange(rows, dtype=jnp.int32)[:, None]
    col_pos = jnp.arange(cols, dtype=jnp.int32)[None, :]
    centre = row_pos * cols // rows
    distance = jnp.abs(col_pos - centre)
    distance = jnp.minimum(distance, cols - distance)
    width = max(cols // 8, 1)
    threshold = 250 + 700 * jnp.maximum(width - distance, 0) // width
    rolled = jax.random.randint(key, (rows, cols), 0, 1000)
    return (rolled < threshold).astype(jnp.int32)


def draw_left_mask(key, part):
    return banded(jax.random.fold_in(key, 11), MB, KB)


def draw_right_mask(key, part):
    return banded(jax.random.fold_in(key, 23), NB, KB).T


def with_ends(result, own_key, low, largest):
    place = [jax.random.randint(jax.random.fold_in(own_key, axis), (), 0, length) for axis, length in enumerate(result.shape)]
    main_axis = result.shape.index(max(result.shape))
    beside = place[:main_axis] + [(place[main_axis] + 1) % result.shape[main_axis]] + place[main_axis + 1:]
    return result.at[tuple(place)].set(low).at[tuple(beside)].set(largest)


def level_of(own_key, extent, cuts, low, largest):
    level, own = 1.0, jax.random.fold_in(own_key, 6)
    for position, shards_of in cuts:
        draws = jnp.exp(jax.random.uniform(jax.random.fold_in(own, position), (shards_of,), jnp.float32, low / len(cuts), largest / len(cuts)))
        level = level * jnp.repeat(draws, extent[position] // shards_of).reshape([-1 if axis == position else 1 for axis in range(len(extent))])
    return level


def gaussian(key, extent, deviation, bound, cuts=(), kind=jnp.bfloat16):
    factor_of = level_of(key, extent, cuts, -0.22, 0.18) if cuts else 1.0
    result = jax.random.normal(key, extent, jnp.float32) * deviation * factor_of
    return jnp.minimum(jnp.maximum(result, -bound), bound).astype(kind)


def setup_inputs(seed: int = 0) -> dict:
    arg_keys = jax.random.split(jax.random.key(seed), 6)
    left_matrix = gaussian(arg_keys[0], (M, ORDER), 1.0, 6.0, ((0, 8), (1, 16)))
    right_matrix = gaussian(arg_keys[1], (ORDER, N), (TICKS * UNIT // 2) ** -0.5, 0.078125, ((0, 8), (1, 16)))
    left_mask = draw_left_mask(jax.random.fold_in(arg_keys[5], 71), 0)
    right_mask = draw_right_mask(jax.random.fold_in(arg_keys[5], 71), 0)
    keep_mask = with_ends((jax.random.randint(arg_keys[4], (MB, NB), 0, 4) < 3).astype(jnp.int32), jax.random.fold_in(arg_keys[4], 1), 0, 1)
    return {"left_matrix": left_matrix, "right_matrix": right_matrix, "left_mask": left_mask, "right_mask": right_mask, "keep_mask": keep_mask}


def sparsify(matrix, mask):
    rows, cols = matrix.shape
    shaped = matrix.reshape(rows // BLOCK, BLOCK, cols // BLOCK, BLOCK)
    return (shaped * mask[:, None, :, None].astype(matrix.dtype)).reshape(rows, cols)


def reference(left_matrix, right_matrix, left_mask, right_mask, keep_mask):
    left_sparse = sparsify(left_matrix, left_mask)
    right_sparse = sparsify(right_matrix, right_mask)
    group_cols = 2 * NC_DEV
    panels = []
    for panel in range(N_ROW):
        pieces = []
        for group in range(N_ROW):
            total = jnp.zeros((MR_DEV, group_cols), jnp.float32)
            for tick in range(TICKS):
                unit = (panel + group + tick) % N_ROW
                left_piece = left_sparse[panel * MR_DEV:(panel + 1) * MR_DEV, unit * UNIT:(unit + 1) * UNIT]
                right_piece = right_sparse[unit * UNIT:(unit + 1) * UNIT, group * group_cols:(group + 1) * group_cols]
                total = total + jnp.dot(left_piece, right_piece, preferred_element_type=jnp.float32)
            pieces.append(total)
        panels.append(jnp.concatenate(pieces, axis=1))
    total_all = jnp.concatenate(panels, axis=0)
    kept = total_all.reshape(MB, BLOCK, NB, BLOCK) * keep_mask[:, None, :, None].astype(jnp.float32)
    return kept.reshape(M, N).astype(jnp.bfloat16)
```

```python
import jax
import jax.numpy as jnp
from jax import lax
from jax.experimental import pallas as pl
from jax.experimental.pallas import tpu as pltpu
from jax.sharding import PartitionSpec as P

BLOCK = 128
TICKS = 3
ROWS = 8
HALF = 4
COLS = 16
UNITS = 8
ROW_CUTS = 2
COL_CUTS = 2


def send(value, route, where=lambda row, col: True):
    pairs = []
    for row in range(ROWS):
        for col in range(COLS):
            if where(row, col):
                to_row, to_col = route(row, col)
                pairs.append((row * COLS + col, to_row * COLS + to_col))
    return lax.ppermute(value, ("row", "col"), pairs)


def at(group, core):
    return 2 * (group % UNITS) + core


def skewed(row, col):
    unit, core = divmod(col, 2)
    first = (unit - row) % UNITS
    if row % 2:
        group = first - 1
    else:
        group = first if first % 2 else first - 2
    return HALF * (unit // HALF) + row % HALF, at(group, core)


def swapped(row, col):
    group, core = divmod(col, 2)
    return row, at(group ^ 1, core)


def lifted(row, col):
    group, core = divmod(col, 2)
    return row, at(group - 2 if group % 2 else group + 2, core)


def partner(row, col):
    return row, col ^ 1


def mirrored(row, col):
    return (row + HALF) % ROWS, col


def along(by):
    return lambda row, col: (row // HALF * HALF + (row + by) % HALF, col)


def sparsify(matrix, mask):
    rows, cols = matrix.shape
    shaped = matrix.reshape(rows // BLOCK, BLOCK, cols // BLOCK, BLOCK)
    return (shaped * mask[:, None, :, None].astype(matrix.dtype)).reshape(rows, cols)


def products(table, lefts, rights):
    rows, depth = lefts[0].shape
    cols = rights[0].shape[1]
    steps = [(piece, half) for piece in range(TICKS) for half in range(2)]

    def kernel(table_ref, *refs):
        left_refs, right_refs = refs[:8], refs[8:13]
        own_ref, mirror_ref, left_buf, right_buf, acc_ref, left_sem, right_sem = refs[13:]
        core, odd = table_ref[0], table_ref[1]

        def left_copy(source, step):
            return pltpu.make_async_copy(source, left_buf.at[step], left_sem.at[step])

        def right_copy(source, step):
            return pltpu.make_async_copy(source, right_buf.at[step], right_sem.at[step])

        for step, (piece, half) in enumerate(steps):
            for other in range(2):
                mine = core == half if other == 0 else core != half
                if piece < 2:
                    @pl.when(mine)
                    def _():
                        left_copy(left_refs[2 * piece + other], step).start()
                else:
                    for parity in range(2):
                        @pl.when(jnp.logical_and(mine, odd == parity))
                        def _():
                            left_copy(left_refs[4 + 2 * parity + other], step).start()
            offset = table_ref[2 + piece]
            for which, ref in ((0, right_refs[0]), (1, right_refs[1]), (3, right_refs[2])):
                @pl.when(offset == which)
                def _():
                    right_copy(ref.at[pl.ds(half * depth, depth), :], step).start()

            @pl.when(offset == 2)
            def _():
                right_copy(right_refs[3 + half], step).start()
        acc_ref[...] = jnp.zeros_like(acc_ref)
        for step, (piece, half) in enumerate(steps):
            left_copy(left_refs[0], step).wait()
            right_copy(right_refs[3], step).wait()
            part = jnp.dot(left_buf[step], right_buf[step], preferred_element_type=jnp.float32)
            acc_ref[table_ref[5 + piece]] += part
        own_ref[...] = acc_ref[0]
        mirror_ref[...] = acc_ref[1]

    hbm = pl.BlockSpec(memory_space=pl.ANY)
    count = len(steps)
    return pl.pallas_call(
        kernel,
        out_shape=[jax.ShapeDtypeStruct((rows, cols), jnp.float32)] * 2,
        in_specs=[pl.BlockSpec(memory_space=pltpu.SMEM)] + [hbm] * 13,
        out_specs=[pl.BlockSpec(memory_space=pltpu.VMEM)] * 2,
        scratch_shapes=[
            pltpu.VMEM((count, rows, depth), jnp.bfloat16),
            pltpu.VMEM((count, depth, cols), jnp.bfloat16),
            pltpu.VMEM((2, rows, cols), jnp.float32),
            pltpu.SemaphoreType.DMA((count,)),
            pltpu.SemaphoreType.DMA((count,)),
        ],
        compiler_params=pltpu.CompilerParams(vmem_limit_bytes=48 << 20),
        cost_estimate=pl.CostEstimate(
            flops=2 * count * rows * depth * cols,
            bytes_accessed=2 * count * depth * (rows + cols),
            transcendentals=0,
        ),
    )(table, *lefts, *rights)


def shards(left_matrix, right_matrix, left_mask, right_mask, keep_mask):
    row = lax.axis_index("row")
    col = lax.axis_index("col")
    high = row % HALF
    group = col // 2
    odd = row % 2
    parity = group % 2
    ticks = [
        jnp.where(odd == 0, jnp.where(parity == 0, 2, 0), 1),
        jnp.where(odd == 0, 1, jnp.where(parity == 0, 2, 0)),
        jnp.where(parity == 0, 0, 2),
    ]
    offsets = [(group + tick) % HALF for tick in ticks]
    sides = [(high + group + tick) // HALF % 2 for tick in ticks]
    table = jnp.stack([col % 2, odd] + offsets + sides).astype(jnp.int32)

    rights = []
    cols = right_matrix.shape[1] // COL_CUTS
    for cut in range(COL_CUTS):
        blocks = cols // BLOCK
        piece = sparsify(
            right_matrix[:, cut * cols:(cut + 1) * cols],
            right_mask[:, cut * blocks:(cut + 1) * blocks],
        )
        after = send(piece, along(-1))
        before = send(piece, along(1))
        depth = piece.shape[0] // 2
        across = (send(before[:depth], along(1)), send(after[depth:], along(-1)))
        rights.append((piece, after, before) + across)

    lefts = []
    rows = left_matrix.shape[0] // ROW_CUTS
    for cut in range(ROW_CUTS):
        blocks = rows // BLOCK
        piece = sparsify(
            left_matrix[cut * rows:(cut + 1) * rows],
            left_mask[cut * blocks:(cut + 1) * blocks],
        )
        first = send(piece, skewed)
        second = send(first, swapped)
        even = send(first, lifted, lambda row, col: row % 2 == 0)
        uneven = send(second, lifted, lambda row, col: row % 2 == 1)
        lefts.append([part for own in (first, second, even, uneven) for part in (own, send(own, partner))])

    bands = []
    for cut in range(ROW_CUTS):
        band = []
        for side in range(COL_CUTS):
            own, mirror = products(table, lefts[cut], rights[side])
            band.append(own + send(mirror, mirrored))
        bands.append(jnp.concatenate(band, axis=1))
    total = jnp.concatenate(bands, axis=0)
    rows, cols = total.shape
    kept = total.reshape(rows // BLOCK, BLOCK, cols // BLOCK, BLOCK) * keep_mask[
        :, None, :, None
    ].astype(jnp.float32)
    return kept.reshape(rows, cols).astype(jnp.bfloat16)


def solution(mesh):
    placed = (P("row", "col"), P("row", "col"), P("row", "col"), P("row", "col"), P("row", "col"))
    return jax.shard_map(
        shards, mesh=mesh, in_specs=placed, out_specs=P("row", "col"), check_vma=False
    )
```
